8 devices in a mesh: side: 2 (over z, y), rep: 4 (over x, core).
Axes of the slice: x: 2, y: 2, z: 1, core: 2. Of those that a mesh axis runs over, the one named last changes fastest.
Arguments:
- w_up: float32 [2, 2, 2048, 6144], P('side', None, 'rep')
- w_down: float32 [2, 2, 6144, 2048], P('side', None, None, 'rep')
- g_up: float32 [2, 2, 2048, 6144], P('side', None, 'rep')
- g_down: float32 [2, 2, 6144, 2048], P('side', None, None, 'rep')
- learn_rate: float32 [], replicated
- prompts: bfloat16 [2, 16384, 2048], P('side', 'rep')
- prompt_lens: int32 [4], P('rep')
Outputs:
- output 1: float32 [2, 2, 2048, 6144], P('side', None, 'rep')
- output 2: float32 [2, 2, 6144, 2048], P('side', None, None, 'rep')
- output 3: bfloat16 [2, 16384, 2048], P('side', 'rep')
All inputs are finite; a program needn't handle non-finite values.
Results may differ from the reference program's by a relative error of at most 0.00783483.
Values are sent between devices in bfloat16 or wider.
A program may use at most 1 GiB of HBM per device.

```python
import jax
import jax.numpy as jnp
from jax import lax

SIDE_DEVS = 2
REP_DEVS = 4
MODEL_DIM = 2048
FFN_DIM = 6144
LAYERS = 2
TOKENS = 4096
TP_WAYS = SIDE_DEVS // 2
FF_PIECE = FFN_DIM // TP_WAYS
D_PIECE = MODEL_DIM // TP_WAYS


def draw_lens(len_key):
    key_a, key_b = jax.random.split(len_key)
    low_len = max(1, TOKENS // 32)
    base_lens = jax.random.randint(key_a, (REP_DEVS,), low_len, TOKENS + 1, jnp.int32)
    full_slot = jax.random.randint(key_b, (), 0, REP_DEVS, jnp.int32)
    return jnp.where(jnp.arange(REP_DEVS) == full_slot, TOKENS, base_lens).astype(jnp.int32)


def setup_inputs(seed: int = 0) -> dict:
    sub_keys = jax.random.split(jax.random.key(seed), 7)
    up_shape = (TP_WAYS, LAYERS, MODEL_DIM, FF_PIECE)
    down_shape = (TP_WAYS, LAYERS, FF_PIECE, MODEL_DIM)
    up_scale = MODEL_DIM ** -0.5
    down_scale = 0.7 * FFN_DIM ** -0.5
    w_up = jax.random.normal(sub_keys[0], up_shape, jnp.float32) * up_scale
    w_down = jax.random.normal(sub_keys[1], down_shape, jnp.float32) * down_scale
    g_up = jax.random.normal(sub_keys[2], up_shape, jnp.float32) * up_scale
    g_down = jax.random.normal(sub_keys[3], down_shape, jnp.float32) * down_scale
    learn_rate = jax.random.uniform(sub_keys[4], (), jnp.float32, 0.02, 0.25)
    gen_rows = jax.random.normal(sub_keys[5], (TP_WAYS, REP_DEVS * TOKENS, D_PIECE), jnp.float32)
    prompts = jnp.concatenate([jnp.zeros_like(gen_rows), gen_rows], axis=0).astype(jnp.bfloat16)
    return {
        "w_up": jnp.concatenate([w_up, jnp.zeros_like(w_up)], axis=0),
        "w_down": jnp.concatenate([w_down, jnp.zeros_like(w_down)], axis=0),
        "g_up": jnp.concatenate([g_up, jnp.zeros_like(g_up)], axis=0),
        "g_down": jnp.concatenate([g_down, jnp.zeros_like(g_down)], axis=0),
        "learn_rate": learn_rate,
        "prompts": prompts,
        "prompt_lens": draw_lens(sub_keys[6]),
    }


def reference(w_up, w_down, g_up, g_down, learn_rate, prompts, prompt_lens):
    new_up = w_up - learn_rate * g_up
    new_down = w_down - learn_rate * g_down
    up_bf = new_up[:TP_WAYS].astype(jnp.bfloat16)
    down_bf = new_down[:TP_WAYS].astype(jnp.bfloat16)
    up_full = jnp.transpose(up_bf, (1, 2, 0, 3)).reshape(LAYERS, MODEL_DIM, FFN_DIM)
    down_full = jnp.transpose(down_bf, (1, 0, 2, 3)).reshape(LAYERS, FFN_DIM, MODEL_DIM)
    x_full = jnp.transpose(prompts[TP_WAYS:], (1, 0, 2)).reshape(REP_DEVS, TOKENS, MODEL_DIM)

    def layer_step(h_rows, layer_w):
        up_layer, down_layer = layer_w
        pre_act = jnp.dot(h_rows, up_layer, preferred_element_type=jnp.float32)
        act_bf = jax.nn.gelu(pre_act, approximate=True).astype(jnp.bfloat16)
        part_sum = jnp.dot(act_bf, down_layer, preferred_element_type=jnp.float32)
        return (h_rows.astype(jnp.float32) + part_sum).astype(jnp.bfloat16), None

    def one_replica(replica_in):
        row_block, length = replica_in
        h_rows, _ = lax.scan(layer_step, row_block, (up_full, down_full))
        keep_mask = jnp.arange(TOKENS)[:, None] < length
        return jnp.where(keep_mask, h_rows, jnp.zeros_like(h_rows))

    y_full = lax.map(one_replica, (x_full, prompt_lens))
    y_gen = jnp.transpose(y_full.reshape(REP_DEVS * TOKENS, TP_WAYS, D_PIECE), (1, 0, 2))
    outputs = jnp.concatenate([jnp.zeros_like(y_gen), y_gen], axis=0)
    return new_up, new_down, outputs
```

```python
import jax
import jax.numpy as jnp
from jax import lax
from jax.experimental import pallas as pl
from jax.experimental.pallas import tpu as pltpu
from jax.sharding import PartitionSpec as P

MESH = pl.DeviceIdType.MESH
LAYERS, DIM, FFN, TOKENS = 2, 2048, 6144, 4096
RANKS = 4
COLS = DIM // RANKS
CHUNK = 512
CHUNKS = LAYERS * FFN // CHUNK
PER_LAYER = FFN // CHUNK
PARTS = 4
PART_ROWS = 2 * CHUNK // PARTS
PIECES = CHUNKS * PARTS
TILE = 512
TILES = TOKENS // TILE
STEPS = CHUNKS * TILES
AHEAD, X_LAG, PAIR_LAG = 12, 3, 1
PER = TILES // PARTS
WINDOW = 4
RING = 8


def update_kernel(lr_ref, w_up, g_up, w_dn, g_dn, new_up, new_dn, sent):
    lr = lr_ref[0]
    up = w_up[...] - lr * g_up[...]
    new_up[...] = up
    dn = w_dn[...] - lr * g_dn[...]
    new_dn[...] = dn
    half = PARTS // 2
    sent[0:half] = up.astype(jnp.bfloat16).reshape(half, PART_ROWS, CHUNK)
    sent[half:PARTS] = dn.astype(jnp.bfloat16).reshape(half, PART_ROWS, COLS)


def update(learn_rate, w_up, g_up, w_dn, g_dn):
    up_spec = pl.BlockSpec((None, None, COLS, CHUNK), lambda c: (0, c // PER_LAYER, 0, c % PER_LAYER))
    dn_spec = pl.BlockSpec((None, None, CHUNK, COLS), lambda c: (0, c // PER_LAYER, c % PER_LAYER, 0))
    return pl.pallas_call(
        update_kernel,
        grid=(CHUNKS,),
        out_shape=(
            jax.ShapeDtypeStruct(w_up.shape, jnp.float32),
            jax.ShapeDtypeStruct(w_dn.shape, jnp.float32),
            jax.ShapeDtypeStruct((PIECES, PART_ROWS, CHUNK), jnp.bfloat16),
        ),
        in_specs=[pl.BlockSpec(memory_space=pltpu.SMEM), up_spec, up_spec, dn_spec, dn_spec],
        out_specs=(up_spec, dn_spec, pl.BlockSpec((PARTS, PART_ROWS, CHUNK), lambda c: (c, 0, 0))),
        cost_estimate=pl.CostEstimate(flops=100_000_000, bytes_accessed=176_000_000, transcendentals=0),
        name="update",
    )(learn_rate.reshape(1), w_up, g_up, w_dn, g_dn)


def gelu(z):
    return 0.5 * z * (1.0 + jnp.tanh(0.7978845608 * (z + 0.044715 * (z * z * z))))


def stack_kernel(
    sent, x_ref, land, y_ref, h, acc, w,
    y_send, y_recv, x_send, x_recv, own_send, own_recv, far_send, far_recv, w_sem, x_sem, out_sem,
):
    side, rep = lax.axis_index("side"), lax.axis_index("rep")
    pair = rep + 1 - 2 * lax.rem(rep, 2)
    cross = lax.rem(rep + 2, RANKS)
    cross_pair = lax.rem(pair + 2, RANKS)
    is_gen = side == 1

    def remote(src, piece, slot, send, recv, to):
        return pltpu.make_async_remote_copy(
            src_ref=src, dst_ref=land.at[piece, slot], send_sem=send, recv_sem=recv,
            device_id=to, device_id_type=MESH,
        )

    def y_copy(p):
        return remote(sent.at[p], p, rep, y_send.at[lax.rem(p, WINDOW)], y_recv.at[p], (1, rep))

    def x_copy(p, slot):
        return remote(land.at[p, slot], p, slot, x_send.at[lax.rem(p, RING)], x_recv.at[p], (1, cross))

    def own_copy(p, slot):
        return remote(land.at[p, slot], p, slot, own_send.at[lax.rem(p, RING)], own_recv.at[p], (1, pair))

    def far_copy(p, slot):
        return remote(land.at[p, slot], p, slot, far_send.at[lax.rem(p, RING)], far_recv.at[p], (1, pair))

    def load(p):
        k = lax.rem(p, PARTS)
        s = lax.rem(p // PARTS, 2)
        return pltpu.make_async_copy(
            land.at[p], w.at[s, k // 2, :, lax.rem(k, 2)], w_sem.at[s, k]
        )

    barrier = pltpu.get_barrier_semaphore()

    @pl.when(side == 0)
    def trainer():
        pl.semaphore_signal(barrier, inc=1, device_id=(1, rep), device_id_type=MESH)
        pl.semaphore_wait(barrier, 1)

        def send(p, _):
            @pl.when(p >= WINDOW)
            def _():
                y_copy(p - WINDOW).wait_send()

            y_copy(p).start()
            return 0

        lax.fori_loop(0, PIECES, send, 0)

        def drain(p, _):
            y_copy(p).wait_send()
            return 0

        lax.fori_loop(PIECES - WINDOW, PIECES, drain, 0)

    @pl.when(is_gen)
    def generator():
        x_in = pltpu.make_async_copy(x_ref, h, x_sem)
        x_in.start()
        for to in ((0, rep), (1, pair), (1, cross)):
            pl.semaphore_signal(barrier, inc=1, device_id=to, device_id_type=MESH)
        pl.semaphore_wait(barrier, 3)

        def rows_of(i):
            return pl.ds(pl.multiple_of(i * TILE, TILE), TILE)

        def out_copy(i):
            return pltpu.make_async_copy(h.at[rows_of(i)], y_ref.at[rows_of(i)], out_sem.at[i])

        def event(s, lag, fn):
            q = s + AHEAD - lag
            p = q // PER
            pl.when((lax.rem(q + PER * PIECES, PER) == 0) & (p >= 0) & (p < PIECES))(lambda: fn(p))

        def on_y(p):
            y_copy(p).wait_recv()

            @pl.when(p >= RING)
            def _():
                x_copy(p - RING, rep).wait_send()
                own_copy(p - RING, rep).wait_send()

            x_copy(p, rep).start()
            own_copy(p, rep).start()

        def on_x(p):
            x_copy(p, cross).wait_recv()

            @pl.when(p >= RING)
            def _():
                far_copy(p - RING, cross).wait_send()

            far_copy(p, cross).start()

        def on_pair(p):
            own_copy(p, pair).wait_recv()
            far_copy(p, cross_pair).wait_recv()
            load(p).start()

        def compute(c, i):
            slot = lax.rem(c, 2)

            @pl.when(i == 0)
            def _():
                for k in range(PARTS):
                    load(c * PARTS + k).wait()

            half = TILE // 2
            first = pl.multiple_of(i * TILE, TILE)
            parts = [pl.ds(first + k * half, half) for k in range(2)]
            pre = [
                jnp.dot(h[rows, :], w[slot, 0].reshape(DIM, CHUNK), preferred_element_type=jnp.float32)
                for rows in parts
            ]
            act = [gelu(z).astype(jnp.bfloat16) for z in pre]
            for rows, u in zip(parts, act):
                for n in range(RANKS):
                    acc[rows, n * COLS:(n + 1) * COLS] += jnp.dot(
                        u, w[slot, 1, n].reshape(CHUNK, COLS), preferred_element_type=jnp.float32
                    )

            rows = rows_of(i)

            @pl.when(lax.rem(c, PER_LAYER) == PER_LAYER - 1)
            def _():
                h[rows, :] = acc[rows, :].astype(jnp.bfloat16)

                @pl.when(c < CHUNKS - 1)
                def _():
                    acc[rows, :] = h[rows, :].astype(jnp.float32)

                @pl.when(c == CHUNKS - 1)
                def _():
                    out_copy(i).start()

        def step(t, _):
            s = t - AHEAD
            event(s, 0, on_y)
            event(s, X_LAG, on_x)
            event(s, X_LAG + PAIR_LAG, on_pair)

            @pl.when((s < 0) & (s >= -TILES))
            def _():
                i = s + TILES

                @pl.when(i == 0)
                def _():
                    x_in.wait()

                acc[rows_of(i), :] = h[rows_of(i), :].astype(jnp.float32)

            @pl.when(s >= 0)
            def _():
                compute(s // TILES, lax.rem(s, TILES))

            return 0

        lax.fori_loop(0, AHEAD + STEPS, step, 0)

        def drain(p, _):
            x_copy(p, rep).wait_send()
            own_copy(p, rep).wait_send()
            far_copy(p, cross).wait_send()
            return 0

        lax.fori_loop(PIECES - RING, PIECES, drain, 0)
        for i in range(TILES):
            out_copy(i).wait()


def mlp_stack(sent, x):
    dma = pltpu.SemaphoreType.DMA
    return pl.pallas_call(
        stack_kernel,
        out_shape=(
            jax.ShapeDtypeStruct((PIECES, RANKS, PART_ROWS, CHUNK), jnp.bfloat16),
            jax.ShapeDtypeStruct((TOKENS, DIM), jnp.bfloat16),
        ),
        in_specs=[pl.BlockSpec(memory_space=pl.ANY)] * 2,
        out_specs=(pl.BlockSpec(memory_space=pl.ANY),) * 2,
        scratch_shapes=[
            pltpu.VMEM((TOKENS, DIM), jnp.bfloat16),
            pltpu.VMEM((TOKENS, DIM), jnp.float32),
            pltpu.VMEM((2, 2, RANKS, PARTS // 2, PART_ROWS, CHUNK), jnp.bfloat16),
            dma((WINDOW,)), dma((PIECES,)),
            dma((RING,)), dma((PIECES,)),
            dma((RING,)), dma((PIECES,)),
            dma((RING,)), dma((PIECES,)),
            dma((2, PARTS)), dma, dma((TILES,)),
        ],
        compiler_params=pltpu.CompilerParams(
            collective_id=0, has_side_effects=True, vmem_limit_bytes=67_043_328
        ),
        cost_estimate=pl.CostEstimate(flops=412_000_000_000, bytes_accessed=300_000_000, transcendentals=50_000_000),
        name="stack",
    )(sent, x)


def solution(mesh):
    up_spec = P("side", None, "rep", None)
    down_spec = P("side", None, None, "rep")
    act_spec = P("side", "rep", None)

    def device_step(w_up, w_down, g_up, g_down, learn_rate, prompts, prompt_lens):
        new_up, new_down, sent = update(learn_rate, w_up, g_up, w_down, g_down)
        _, y = mlp_stack(sent, prompts[0])
        keep = (jnp.arange(TOKENS)[:, None] < prompt_lens[0]) & (lax.axis_index("side") == 1)
        return new_up, new_down, jnp.where(keep, y, jnp.zeros_like(y))[None]

    return jax.shard_map(
        device_step,
        mesh=mesh,
        in_specs=(up_spec, down_spec, up_spec, down_spec, P(), act_spec, P("rep")),
        out_specs=(up_spec, down_spec, act_spec),
        check_vma=False,
    )
```

```python
import jax
import jax.numpy as jnp
from jax import lax
from jax.experimental import pallas as pl
from jax.experimental.pallas import tpu as pltpu
from jax.sharding import PartitionSpec as P

MESH = pl.DeviceIdType.MESH
LAYERS, DIM, FFN, TOKENS = 2, 2048, 6144, 4096
RANKS = 4
COLS = DIM // RANKS
CHUNK = 512
CHUNKS = LAYERS * FFN // CHUNK
PER_LAYER = FFN // CHUNK
PARTS = 4
PART_ROWS = 2 * CHUNK // PARTS
PIECES = CHUNKS * PARTS
TILE = 512
TILES = TOKENS // TILE
LAST = CHUNKS - 1
STEPS = LAST * TILES
AHEAD, X_LAG, PAIR_LAG = 12, 3, 1
PER = TILES // PARTS
WINDOW = 4
RING = 8
STAGES = 3
HELD = 56
BACK = 8
HALF = TILE // 2
STACK_VMEM = 8_300_000


def gelu(z):
    return 0.5 * z * (1.0 + jnp.tanh(0.7978845608 * (z + 0.044715 * (z * z * z))))


def piece_of(up_ref, dn_ref, c, k):
    layer, col = c // PER_LAYER, lax.rem(c, PER_LAYER) * CHUNK
    if k < PARTS // 2:
        cols = pl.ds(pl.multiple_of(col, CHUNK), CHUNK)
        return up_ref.at[0, layer, pl.ds(k * PART_ROWS, PART_ROWS), cols]
    first = pl.multiple_of(col + (k - PARTS // 2) * PART_ROWS, PART_ROWS)
    return dn_ref.at[0, layer, pl.ds(first, PART_ROWS), :]


def held_piece(acc, c, k):
    return acc.at[pl.ds(pl.multiple_of(c * PART_ROWS, PART_ROWS), PART_ROWS), pl.ds(k * CHUNK, CHUNK)]


def stage(acc, s):
    first = pl.multiple_of((HELD + s) // PARTS * PART_ROWS, PART_ROWS)
    col = pl.multiple_of(lax.rem(s, PARTS) * CHUNK, CHUNK)
    return acc.at[pl.ds(first, PART_ROWS), pl.ds(col, CHUNK)]


def rows_of(i):
    return pl.ds(pl.multiple_of(i * TILE, TILE), TILE)


def up_act(h, w_up, i):
    first = pl.multiple_of(i * TILE, TILE)
    parts = [pl.ds(first + k * HALF, HALF) for k in range(2)]
    pre = [
        jnp.dot(h[rows, :], w_up.reshape(DIM, CHUNK), preferred_element_type=jnp.float32)
        for rows in parts
    ]
    return [(rows, gelu(z).astype(jnp.bfloat16)) for rows, z in zip(parts, pre)]


def stack_kernel(
    lr_ref, lens, w_up, g_up, w_dn, g_dn, x_ref, land, left, h, acc, w,
    y_send, y_recv, x_send, x_recv, own_send, own_recv, far_send, far_recv,
    w_sem, x_sem, w_in, g_in, left_sem,
):
    del lens
    side, rep = lax.axis_index("side"), lax.axis_index("rep")
    pair = rep + 1 - 2 * lax.rem(rep, 2)
    cross = lax.rem(rep + 2, RANKS)
    cross_pair = lax.rem(pair + 2, RANKS)

    def remote(src, piece, slot, send, recv, to):
        return pltpu.make_async_remote_copy(
            src_ref=src, dst_ref=land.at[piece, slot], send_sem=send, recv_sem=recv,
            device_id=to, device_id_type=MESH,
        )

    def y_copy(p):
        s = lax.rem(p, RING)
        src = w.at[0, s // 4, lax.rem(s, 4), 0]
        return remote(src, p, rep, y_send.at[lax.rem(p, WINDOW)], y_recv.at[p], (1, rep))

    def x_copy(p, slot):
        return remote(land.at[p, slot], p, slot, x_send.at[lax.rem(p, RING)], x_recv.at[p], (1, cross))

    def own_copy(p, slot):
        return remote(land.at[p, slot], p, slot, own_send.at[lax.rem(p, RING)], own_recv.at[p], (1, pair))

    def far_copy(p, slot):
        return remote(land.at[p, slot], p, slot, far_send.at[lax.rem(p, RING)], far_recv.at[p], (1, pair))

    def load(p):
        k = lax.rem(p, PARTS)
        s = lax.rem(p // PARTS, 2)
        return pltpu.make_async_copy(
            land.at[p], w.at[s, k // 2, :, lax.rem(k, 2)], w_sem.at[s, k]
        )

    barrier = pltpu.get_barrier_semaphore()

    @pl.when(side == 0)
    def trainer():
        def w_stage(s):
            return stage(acc, s)

        def g_stage(s):
            return stage(acc, PARTS + s)

        def fetch(c, k):
            s = lax.rem(c * PARTS + k, STAGES)
            return (
                pltpu.make_async_copy(piece_of(w_up, w_dn, c, k), w_stage(s), w_in.at[s]),
                pltpu.make_async_copy(piece_of(g_up, g_dn, c, k), g_stage(s), g_in.at[s]),
            )

        def spill(p):
            s = lax.rem(p, STAGES)
            return pltpu.make_async_copy(w_stage(s), left.at[p - HELD], left_sem.at[s])

        for k in range(2):
            for copy in fetch(0, k):
                copy.start()
        pl.semaphore_signal(barrier, inc=1, device_id=(1, rep), device_id_type=MESH)
        pl.semaphore_wait(barrier, 1)
        lr = lr_ref[0]

        def send(p):
            @pl.when(p >= WINDOW)
            def _():
                y_copy(p - WINDOW).wait_send()

            y_copy(p).start()

        def chunk(c, _):
            for k in range(PARTS):
                p = c * PARTS + k
                for copy in fetch(c, k):
                    copy.wait()
                s = lax.rem(p, STAGES)
                new = w_stage(s)[...] - lr * g_stage(s)[...]
                r = lax.rem(p, RING)
                w[0, r // 4, lax.rem(r, 4), 0] = new.astype(jnp.bfloat16)

                @pl.when(p < HELD)
                def _():
                    held_piece(acc, c, k)[...] = new

                @pl.when(p >= HELD)
                def _():
                    w_stage(s)[...] = new

                @pl.when(p >= 1)
                def _():
                    send(p - 1)

                @pl.when(p - 1 >= HELD)
                def _():
                    spill(p - 1).start()
                    spill(p - 1).wait()

                ahead = k + 2

                @pl.when(p + 2 < PIECES)
                def _():
                    for copy in fetch(c + ahead // PARTS, ahead % PARTS):
                        copy.start()

            return 0

        lax.fori_loop(0, CHUNKS, chunk, 0)
        send(PIECES - 1)
        spill(PIECES - 1).start()
        spill(PIECES - 1).wait()

        def drain(p, _):
            y_copy(p).wait_send()
            return 0

        lax.fori_loop(PIECES - WINDOW, PIECES, drain, 0)

    @pl.when(side == 1)
    def generator():
        x_in = pltpu.make_async_copy(x_ref, h, x_sem)
        x_in.start()
        for to in ((0, rep), (1, pair), (1, cross)):
            pl.semaphore_signal(barrier, inc=1, device_id=to, device_id_type=MESH)
        pl.semaphore_wait(barrier, 3)

        def event(s, lag, fn):
            q = s + AHEAD - lag
            p = q // PER
            pl.when((lax.rem(q + PER * PIECES, PER) == 0) & (p >= 0) & (p < PIECES))(lambda: fn(p))

        def on_y(p):
            y_copy(p).wait_recv()

            @pl.when(p >= RING)
            def _():
                x_copy(p - RING, rep).wait_send()
                own_copy(p - RING, rep).wait_send()

            x_copy(p, rep).start()
            own_copy(p, rep).start()

        def on_x(p):
            x_copy(p, cross).wait_recv()

            @pl.when(p >= RING)
            def _():
                far_copy(p - RING, cross).wait_send()

            far_copy(p, cross).start()

        def on_pair(p):
            own_copy(p, pair).wait_recv()
            far_copy(p, cross_pair).wait_recv()
            load(p).start()

        def compute(c, i):
            slot = lax.rem(c, 2)

            @pl.when(i == 0)
            def _():
                for k in range(PARTS):
                    load(c * PARTS + k).wait()

            for rows, u in up_act(h, w[slot, 0], i):
                for n in range(RANKS):
                    acc[rows, n * COLS:(n + 1) * COLS] += jnp.dot(
                        u, w[slot, 1, n].reshape(CHUNK, COLS), preferred_element_type=jnp.float32
                    )

            rows = rows_of(i)

            @pl.when(lax.rem(c, PER_LAYER) == PER_LAYER - 1)
            def _():
                h[rows, :] = acc[rows, :].astype(jnp.bfloat16)
                acc[rows, :] = h[rows, :].astype(jnp.float32)

        def step(t, _):
            s = t - AHEAD
            event(s, 0, on_y)
            event(s, X_LAG, on_x)
            event(s, X_LAG + PAIR_LAG, on_pair)

            @pl.when((s < 0) & (s >= -TILES))
            def _():
                i = s + TILES

                @pl.when(i == 0)
                def _():
                    x_in.wait()

                acc[rows_of(i), :] = h[rows_of(i), :].astype(jnp.float32)

            @pl.when(s >= 0)
            def _():
                compute(s // TILES, lax.rem(s, TILES))

            return 0

        lax.fori_loop(0, AHEAD + STEPS, step, 0)

        def drain(p, _):
            x_copy(p, rep).wait_send()
            own_copy(p, rep).wait_send()
            far_copy(p, cross).wait_send()
            return 0

        lax.fori_loop(PIECES - RING, PIECES, drain, 0)
        for k in range(PARTS):
            load(LAST * PARTS + k).wait()


def mlp_stack(lr, lens, w_up, g_up, w_dn, g_dn, x):
    dma = pltpu.SemaphoreType.DMA
    hbm = pl.BlockSpec(memory_space=pl.ANY)
    vmem = pl.BlockSpec(memory_space=pltpu.VMEM)
    return pl.pallas_call(
        stack_kernel,
        out_shape=(
            jax.ShapeDtypeStruct((PIECES, RANKS, PART_ROWS, CHUNK), jnp.bfloat16),
            jax.ShapeDtypeStruct((PIECES - HELD, PART_ROWS, CHUNK), jnp.float32),
            pltpu.VMEM((TOKENS, DIM), jnp.bfloat16),
            pltpu.VMEM((TOKENS, DIM), jnp.float32),
            pltpu.VMEM((2, 2, RANKS, PARTS // 2, PART_ROWS, CHUNK), jnp.bfloat16),
        ),
        in_specs=[pl.BlockSpec(memory_space=pltpu.SMEM)] * 2 + [hbm] * 5,
        out_specs=(hbm, hbm, vmem, vmem, vmem),
        scratch_shapes=[
            dma((WINDOW,)), dma((PIECES,)),
            dma((RING,)), dma((PIECES,)),
            dma((RING,)), dma((PIECES,)),
            dma((RING,)), dma((PIECES,)),
            dma((2, PARTS)), dma, dma((STAGES,)), dma((STAGES,)), dma((STAGES,)),
        ],
        compiler_params=pltpu.CompilerParams(
            collective_id=0, has_side_effects=True, vmem_limit_bytes=STACK_VMEM
        ),
        cost_estimate=pl.CostEstimate(flops=400_000_000_000, bytes_accessed=300_000_000, transcendentals=50_000_000),
        name="stack",
    )(lr, lens, w_up, g_up, w_dn, g_dn, x)


def last_kernel(
    lens, left, h_in, acc_in, w, new_up, new_dn, y_ref, h, acc, zero, zero_sem, held_sem, back_in, back_out, y_sem
):
    del h_in, acc_in
    side = lax.axis_index("side")

    def y_copy(slot, j):
        rows = pl.ds(pl.multiple_of(j * HALF, HALF), HALF)
        return pltpu.make_async_copy(
            h.at[pl.ds(pl.multiple_of(slot * HALF, HALF), HALF)], y_ref.at[0, rows], y_sem
        )

    @pl.when(side == 0)
    def trainer():
        def held_copy(c, k):
            return pltpu.make_async_copy(held_piece(acc, c, k), piece_of(new_up, new_dn, c, k), held_sem)

        def each(lo, hi, fn):
            def body(c, _):
                for k in range(PARTS):
                    fn(c, k)
                return 0

            lax.fori_loop(lo, hi, body, 0)

        def back_read(c, k):
            b = lax.rem(c, BACK // PARTS) * PARTS + k
            return pltpu.make_async_copy(left.at[c * PARTS + k - HELD], stage(acc, b), back_in.at[b])

        def back_write(c, k):
            b = lax.rem(c, BACK // PARTS) * PARTS + k
            return pltpu.make_async_copy(stage(acc, b), piece_of(new_up, new_dn, c, k), back_out.at[b])

        held = HELD // PARTS
        each(held, held + BACK // PARTS, lambda c, k: back_read(c, k).start())
        each(0, held, lambda c, k: held_copy(c, k).start())
        h[0:HALF, :] = jnp.zeros((HALF, DIM), jnp.bfloat16)

        def bring(c, _):
            for k in range(PARTS):
                back_read(c, k).wait()
                back_write(c, k).start()

            @pl.when((c > held) & (c + 1 < CHUNKS))
            def _():
                for k in range(PARTS):
                    back_write(c - 1, k).wait()
                    back_read(c + 1, k).start()

            return 0

        lax.fori_loop(held, CHUNKS, bring, 0)
        for j in range(2 * TILES):
            y_copy(0, j).start()
        each(0, held, lambda c, k: held_copy(c, k).wait())
        each(CHUNKS - 2, CHUNKS, lambda c, k: back_write(c, k).wait())
        for j in range(2 * TILES):
            y_copy(0, j).wait()

    @pl.when(side == 1)
    def generator():
        zero[...] = jnp.zeros_like(zero)

        def each_zero(fn):
            def body(c, _):
                for k in range(PARTS):
                    fn(pltpu.make_async_copy(zero, piece_of(new_up, new_dn, c, k), zero_sem))
                return 0

            lax.fori_loop(0, CHUNKS, body, 0)

        length = lens[0]
        slot = LAST % 2

        def step(i, _):
            for k, (rows, u) in enumerate(up_act(h, w[slot, 0], i)):
                j = 2 * i + k
                at = lax.broadcasted_iota(jnp.int32, (HALF, COLS), 0) + j * HALF
                for n in range(RANKS):
                    cols = slice(n * COLS, (n + 1) * COLS)
                    total = acc[rows, cols] + jnp.dot(
                        u, w[slot, 1, n].reshape(CHUNK, COLS), preferred_element_type=jnp.float32
                    )
                    h[rows, cols] = jnp.where(at < length, total, 0.0).astype(jnp.bfloat16)

            @pl.when(i == 0)
            def _():
                each_zero(lambda copy: copy.start())

            @pl.when(i >= 1)
            def _():
                y_copy(2 * i - 2, 2 * i - 2).start()
                y_copy(2 * i - 1, 2 * i - 1).start()

            return 0

        lax.fori_loop(0, TILES, step, 0)
        for j in range(2 * TILES - 2, 2 * TILES):
            y_copy(j, j).start()
        each_zero(lambda copy: copy.wait())
        for j in range(2 * TILES):
            y_copy(j, j).wait()


def last_step(lens, left, h, acc, w, up_shape, dn_shape, y_shape):
    dma = pltpu.SemaphoreType.DMA
    hbm = pl.BlockSpec(memory_space=pl.ANY)
    vmem = pl.BlockSpec(memory_space=pltpu.VMEM)
    h, acc, w = (pltpu.with_memory_space_constraint(v, pltpu.VMEM) for v in (h, acc, w))
    new_up, new_dn, y, _, _ = pl.pallas_call(
        last_kernel,
        out_shape=(
            jax.ShapeDtypeStruct(up_shape, jnp.float32),
            jax.ShapeDtypeStruct(dn_shape, jnp.float32),
            jax.ShapeDtypeStruct(y_shape, jnp.bfloat16),
            pltpu.VMEM((TOKENS, DIM), jnp.bfloat16),
            pltpu.VMEM((TOKENS, DIM), jnp.float32),
        ),
        in_specs=[pl.BlockSpec(memory_space=pltpu.SMEM), hbm, vmem, vmem, vmem],
        out_specs=(hbm, hbm, hbm, vmem, vmem),
        input_output_aliases={2: 3, 3: 4},
        scratch_shapes=[
            pltpu.VMEM((PART_ROWS, CHUNK), jnp.float32),
            dma, dma, dma((BACK,)), dma((BACK,)), dma,
        ],
        compiler_params=pltpu.CompilerParams(vmem_limit_bytes=STACK_VMEM),
        cost_estimate=pl.CostEstimate(flops=18_000_000_000, bytes_accessed=67_000_000, transcendentals=2_000_000),
        name="last",
    )(lens, left, h, acc, w)
    return new_up, new_dn, y


def solution(mesh):
    up_spec = P("side", None, "rep", None)
    down_spec = P("side", None, None, "rep")
    act_spec = P("side", "rep", None)

    def device_step(w_up, w_down, g_up, g_down, learn_rate, prompts, prompt_lens):
        _, left, h, acc, w = mlp_stack(
            learn_rate.reshape(1), prompt_lens, w_up, g_up, w_down, g_down, prompts[0]
        )
        return last_step(prompt_lens, left, h, acc, w, w_up.shape, w_down.shape, prompts.shape)

    return jax.shard_map(
        device_step,
        mesh=mesh,
        in_specs=(up_spec, down_spec, up_spec, down_spec, P(), act_spec, P("rep")),
        out_specs=(up_spec, down_spec, act_spec),
        check_vma=False,
    )
```

```python
import jax
import jax.numpy as jnp
from jax import lax
from jax.experimental import pallas as pl
from jax.experimental.pallas import tpu as pltpu
from jax.sharding import PartitionSpec as P

MESH = pl.DeviceIdType.MESH
LAYERS, DIM, FFN, TOKENS = 2, 2048, 6144, 4096
RANKS = 4
COLS = DIM // RANKS
CHUNK = 512
CHUNKS = LAYERS * FFN // CHUNK
PER_LAYER = FFN // CHUNK
PARTS = 4
PART_ROWS = 2 * CHUNK // PARTS
PIECES = CHUNKS * PARTS
BLOCK = 256
TILE = 1024
TILES = TOKENS // TILE
PHASE = TILES
LAST = CHUNKS - 1
STEPS = LAST * 2 * PHASE + PHASE
AHEAD, X_LAG, PAIR_LAG = 7, 3, 1
PER = 2 * PHASE // PARTS
WINDOW = 4
RING = 8
STAGES = 3
HELD = 56
BACK = 8
OUT_TILE = 512
UP_BLOCKS, DOWN_BLOCKS = 4, 4
STACK_VMEM = 8_300_000


def gelu(z):
    return 0.5 * z * (1.0 + jnp.tanh(0.7978845608 * (z + 0.044715 * (z * z * z))))


def piece_of(up_ref, dn_ref, c, k):
    layer, col = c // PER_LAYER, lax.rem(c, PER_LAYER) * CHUNK
    if k < PARTS // 2:
        cols = pl.ds(pl.multiple_of(col, CHUNK), CHUNK)
        return up_ref.at[0, layer, pl.ds(k * PART_ROWS, PART_ROWS), cols]
    first = pl.multiple_of(col + (k - PARTS // 2) * PART_ROWS, PART_ROWS)
    return dn_ref.at[0, layer, pl.ds(first, PART_ROWS), :]


def held_piece(acc, c, k):
    return acc.at[pl.ds(pl.multiple_of(c * PART_ROWS, PART_ROWS), PART_ROWS), pl.ds(k * CHUNK, CHUNK)]


def stage(acc, s):
    first = pl.multiple_of((HELD + s) // PARTS * PART_ROWS, PART_ROWS)
    col = pl.multiple_of(lax.rem(s, PARTS) * CHUNK, CHUNK)
    return acc.at[pl.ds(first, PART_ROWS), pl.ds(col, CHUNK)]


def block_rows(b):
    return pl.ds(pl.multiple_of(b * BLOCK, BLOCK), BLOCK)


def down_cols(n):
    return slice(n * COLS, (n + 1) * COLS)


def down(u, wd, b, n):
    return jnp.dot(u[b], wd[n].reshape(CHUNK, COLS), preferred_element_type=jnp.float32)


def stack_kernel(
    lr_ref, lens, w_up, g_up, w_dn, g_dn, x_ref, land, left, h, acc, u, wu, wd,
    y_send, y_recv, x_send, x_recv, own_send, own_recv, far_send, far_recv,
    w_sem, x_sem, w_in, g_in, left_sem,
):
    del lens
    side, rep = lax.axis_index("side"), lax.axis_index("rep")
    pair = rep + 1 - 2 * lax.rem(rep, 2)
    cross = lax.rem(rep + 2, RANKS)
    cross_pair = lax.rem(pair + 2, RANKS)

    def remote(src, piece, slot, send, recv, to):
        return pltpu.make_async_remote_copy(
            src_ref=src, dst_ref=land.at[piece, slot], send_sem=send, recv_sem=recv,
            device_id=to, device_id_type=MESH,
        )

    def y_copy(p):
        return remote(u.at[lax.rem(p, RING)], p, rep, y_send.at[lax.rem(p, WINDOW)], y_recv.at[p], (1, rep))

    def x_copy(p, slot):
        return remote(land.at[p, slot], p, slot, x_send.at[lax.rem(p, RING)], x_recv.at[p], (1, cross))

    def own_copy(p, slot):
        return remote(land.at[p, slot], p, slot, own_send.at[lax.rem(p, RING)], own_recv.at[p], (1, pair))

    def far_copy(p, slot):
        return remote(land.at[p, slot], p, slot, far_send.at[lax.rem(p, RING)], far_recv.at[p], (1, pair))

    def load(p, k):
        half = PARTS // 2
        to = wu.at[:, k] if k < half else wd.at[:, k - half]
        return pltpu.make_async_copy(land.at[p], to, w_sem.at[k])

    barrier = pltpu.get_barrier_semaphore()

    @pl.when(side == 0)
    def trainer():
        def w_stage(s):
            return stage(acc, s)

        def g_stage(s):
            return stage(acc, PARTS + s)

        def fetch(c, k):
            s = lax.rem(c * PARTS + k, STAGES)
            return (
                pltpu.make_async_copy(piece_of(w_up, w_dn, c, k), w_stage(s), w_in.at[s]),
                pltpu.make_async_copy(piece_of(g_up, g_dn, c, k), g_stage(s), g_in.at[s]),
            )

        def spill(p):
            s = lax.rem(p, STAGES)
            return pltpu.make_async_copy(w_stage(s), left.at[p - HELD], left_sem.at[s])

        for k in range(2):
            for copy in fetch(0, k):
                copy.start()
        pl.semaphore_signal(barrier, inc=1, device_id=(1, rep), device_id_type=MESH)
        pl.semaphore_wait(barrier, 1)
        lr = lr_ref[0]

        def send(p):
            @pl.when(p >= WINDOW)
            def _():
                y_copy(p - WINDOW).wait_send()

            y_copy(p).start()

        def chunk(c, _):
            for k in range(PARTS):
                p = c * PARTS + k
                for copy in fetch(c, k):
                    copy.wait()
                s = lax.rem(p, STAGES)
                new = w_stage(s)[...] - lr * g_stage(s)[...]
                u[lax.rem(p, RING)] = new.astype(jnp.bfloat16)

                @pl.when(p < HELD)
                def _():
                    held_piece(acc, c, k)[...] = new

                @pl.when(p >= HELD)
                def _():
                    w_stage(s)[...] = new

                @pl.when(p >= 1)
                def _():
                    send(p - 1)

                @pl.when(p - 1 >= HELD)
                def _():
                    spill(p - 1).start()
                    spill(p - 1).wait()

                ahead = k + 2

                @pl.when(p + 2 < PIECES)
                def _():
                    for copy in fetch(c + ahead // PARTS, ahead % PARTS):
                        copy.start()

            return 0

        lax.fori_loop(0, CHUNKS, chunk, 0)
        send(PIECES - 1)
        spill(PIECES - 1).start()
        spill(PIECES - 1).wait()

        def drain(p, _):
            y_copy(p).wait_send()
            return 0

        lax.fori_loop(PIECES - WINDOW, PIECES, drain, 0)

    @pl.when(side == 1)
    def generator():
        x_in = pltpu.make_async_copy(x_ref, h, x_sem)
        x_in.start()
        for to in ((0, rep), (1, pair), (1, cross)):
            pl.semaphore_signal(barrier, inc=1, device_id=to, device_id_type=MESH)
        pl.semaphore_wait(barrier, 3)

        def event(s, lag, fn):
            q = s + AHEAD - lag
            p = q // PER
            pl.when((lax.rem(q + PER * PIECES, PER) == 0) & (p >= 0) & (p < PIECES))(lambda: fn(p))

        def on_y(p):
            y_copy(p).wait_recv()

            @pl.when(p >= RING)
            def _():
                x_copy(p - RING, rep).wait_send()
                own_copy(p - RING, rep).wait_send()

            x_copy(p, rep).start()
            own_copy(p, rep).start()

        def on_x(p):
            x_copy(p, cross).wait_recv()

            @pl.when(p >= RING)
            def _():
                far_copy(p - RING, cross).wait_send()

            far_copy(p, cross).start()

        def on_pair(p):
            own_copy(p, pair).wait_recv()
            far_copy(p, cross_pair).wait_recv()
            for k in range(PARTS):
                pl.when(lax.rem(p, PARTS) == k)(lambda k=k: load(p, k).start())

        def up_phase(c, i):
            @pl.when(i == 0)
            def _():
                for k in range(PARTS // 2):
                    load(c * PARTS + k, k).wait()

            def some(g, _):
                blocks = [i * (TILE // BLOCK) + g * UP_BLOCKS + j for j in range(UP_BLOCKS)]
                pre = [
                    jnp.dot(h[block_rows(b), :], wu[...].reshape(DIM, CHUNK), preferred_element_type=jnp.float32)
                    for b in blocks
                ]
                for b, z in zip(blocks, pre):
                    u[b] = gelu(z).astype(jnp.bfloat16)
                return 0

            lax.fori_loop(0, TILE // BLOCK // UP_BLOCKS, some, 0)

        def down_phase(c, i):
            @pl.when(i == 0)
            def _():
                for k in range(PARTS // 2, PARTS):
                    load(c * PARTS + k, k).wait()

            def some(g, _):
                for j in range(DOWN_BLOCKS):
                    b = i * (TILE // BLOCK) + g * DOWN_BLOCKS + j
                    for n in range(RANKS):
                        acc[block_rows(b), down_cols(n)] += down(u, wd, b, n)
                return 0

            lax.fori_loop(0, TILE // BLOCK // DOWN_BLOCKS, some, 0)

            @pl.when(lax.rem(c, PER_LAYER) == PER_LAYER - 1)
            def _():
                lax.fori_loop(0, TILE // BLOCK, lambda j, _: next_h(i * (TILE // BLOCK) + j), 0)

        def next_h(b):
            h[block_rows(b), :] = acc[block_rows(b), :].astype(jnp.bfloat16)
            acc[block_rows(b), :] = h[block_rows(b), :].astype(jnp.float32)
            return 0

        def first_acc(b):
            acc[block_rows(b), :] = h[block_rows(b), :].astype(jnp.float32)
            return 0

        def step(t, _):
            s = t - AHEAD
            event(s, 0, on_y)
            event(s, X_LAG, on_x)
            event(s, X_LAG + PAIR_LAG, on_pair)

            @pl.when((s < 0) & (s >= -TILES))
            def _():
                i = s + TILES

                @pl.when(i == 0)
                def _():
                    x_in.wait()

                lax.fori_loop(0, TILE // BLOCK, lambda j, _: first_acc(i * (TILE // BLOCK) + j), 0)

            c, i = s // (2 * PHASE), lax.rem(s + 2 * PHASE, 2 * PHASE)

            @pl.when((s >= 0) & (i < PHASE))
            def _():
                up_phase(c, i)

            @pl.when((s >= 0) & (i >= PHASE))
            def _():
                down_phase(c, i - PHASE)

            return 0

        lax.fori_loop(0, AHEAD + STEPS, step, 0)

        def drain(p, _):
            x_copy(p, rep).wait_send()
            own_copy(p, rep).wait_send()
            far_copy(p, cross).wait_send()
            return 0

        lax.fori_loop(PIECES - RING, PIECES, drain, 0)
        for k in range(PARTS // 2, PARTS):
            load(LAST * PARTS + k, k).wait()


def mlp_stack(lr, lens, w_up, g_up, w_dn, g_dn, x):
    dma = pltpu.SemaphoreType.DMA
    hbm = pl.BlockSpec(memory_space=pl.ANY)
    vmem = pl.BlockSpec(memory_space=pltpu.VMEM)
    return pl.pallas_call(
        stack_kernel,
        out_shape=(
            jax.ShapeDtypeStruct((PIECES, RANKS, PART_ROWS, CHUNK), jnp.bfloat16),
            jax.ShapeDtypeStruct((PIECES - HELD, PART_ROWS, CHUNK), jnp.float32),
            pltpu.VMEM((TOKENS, DIM), jnp.bfloat16),
            pltpu.VMEM((TOKENS, DIM), jnp.float32),
            pltpu.VMEM((TOKENS // BLOCK, BLOCK, CHUNK), jnp.bfloat16),
            pltpu.VMEM((RANKS, PARTS // 2, PART_ROWS, CHUNK), jnp.bfloat16),
            pltpu.VMEM((RANKS, PARTS // 2, PART_ROWS, COLS), jnp.bfloat16),
        ),
        in_specs=[pl.BlockSpec(memory_space=pltpu.SMEM)] * 2 + [hbm] * 5,
        out_specs=(hbm, hbm) + (vmem,) * 5,
        scratch_shapes=[
            dma((WINDOW,)), dma((PIECES,)),
            dma((RING,)), dma((PIECES,)),
            dma((RING,)), dma((PIECES,)),
            dma((RING,)), dma((PIECES,)),
            dma((PARTS,)), dma, dma((STAGES,)), dma((STAGES,)), dma((STAGES,)),
        ],
        compiler_params=pltpu.CompilerParams(
            collective_id=0, has_side_effects=True, vmem_limit_bytes=STACK_VMEM
        ),
        cost_estimate=pl.CostEstimate(flops=400_000_000_000, bytes_accessed=300_000_000, transcendentals=50_000_000),
        name="stack",
    )(lr, lens, w_up, g_up, w_dn, g_dn, x)


def last_kernel(
    lens, left, h_in, acc_in, u, wd, new_up, new_dn, y_ref, h, acc, zero,
    zero_sem, held_sem, back_in, back_out, y_sem,
):
    del h_in
    side = lax.axis_index("side")

    def y_copy(src, b):
        return pltpu.make_async_copy(h.at[block_rows(src)], y_ref.at[0, block_rows(b)], y_sem)

    @pl.when(side == 0)
    def trainer():
        def held_copy(c, k):
            return pltpu.make_async_copy(held_piece(acc_in, c, k), piece_of(new_up, new_dn, c, k), held_sem)

        def each(lo, hi, fn):
            def body(c, _):
                for k in range(PARTS):
                    fn(c, k)
                return 0

            lax.fori_loop(lo, hi, body, 0)

        def back_read(c, k):
            b = lax.rem(c, BACK // PARTS) * PARTS + k
            return pltpu.make_async_copy(left.at[c * PARTS + k - HELD], stage(acc, b), back_in.at[b])

        def back_write(c, k):
            b = lax.rem(c, BACK // PARTS) * PARTS + k
            return pltpu.make_async_copy(stage(acc, b), piece_of(new_up, new_dn, c, k), back_out.at[b])

        held, blocks = HELD // PARTS, TOKENS // BLOCK
        each(held, held + BACK // PARTS, lambda c, k: back_read(c, k).start())
        h[block_rows(0), :] = jnp.zeros((BLOCK, DIM), jnp.bfloat16)

        def bring(c, _):
            for a in (c - held, c - held + CHUNKS - held):
                @pl.when(a < held)
                def _():
                    for k in range(PARTS):
                        held_copy(a, k).start()

            for k in range(PARTS):
                back_read(c, k).wait()
                back_write(c, k).start()

            @pl.when((c > held) & (c + 1 < CHUNKS))
            def _():
                for k in range(PARTS):
                    back_write(c - 1, k).wait()
                    back_read(c + 1, k).start()

            for b in (2 * (c - held), 2 * (c - held) + 1):
                @pl.when(b < blocks)
                def _():
                    y_copy(0, b).start()

            return 0

        lax.fori_loop(held, CHUNKS, bring, 0)
        each(0, held, lambda c, k: held_copy(c, k).wait())
        each(CHUNKS - 2, CHUNKS, lambda c, k: back_write(c, k).wait())
        for b in range(blocks):
            y_copy(0, b).wait()

    @pl.when(side == 1)
    def generator():
        zero[...] = jnp.zeros_like(zero)

        def each_zero(fn):
            def body(c, _):
                for k in range(PARTS):
                    fn(pltpu.make_async_copy(zero, piece_of(new_up, new_dn, c, k), zero_sem))
                return 0

            lax.fori_loop(0, CHUNKS, body, 0)

        each_zero(lambda copy: copy.start())
        length = lens[0]
        per = OUT_TILE // BLOCK

        def send(i):
            for j in range(per):
                y_copy(i * per + j, i * per + j).start()

        def step(i, _):
            for j in range(per):
                b = i * per + j
                at = lax.broadcasted_iota(jnp.int32, (BLOCK, COLS), 0) + b * BLOCK
                for n in range(RANKS):
                    total = acc_in[block_rows(b), down_cols(n)] + down(u, wd, b, n)
                    h[block_rows(b), down_cols(n)] = jnp.where(at < length, total, 0.0).astype(jnp.bfloat16)

            pl.when(i >= 1)(lambda: send(i - 1))
            return 0

        steps = TOKENS // OUT_TILE
        lax.fori_loop(0, steps, step, 0)
        send(steps - 1)
        each_zero(lambda copy: copy.wait())
        for b in range(TOKENS // BLOCK):
            y_copy(b, b).wait()


def last_step(lens, left, h, acc, u, wd, up_shape, dn_shape, y_shape):
    dma = pltpu.SemaphoreType.DMA
    hbm = pl.BlockSpec(memory_space=pl.ANY)
    vmem = pl.BlockSpec(memory_space=pltpu.VMEM)
    h, acc, u, wd = (pltpu.with_memory_space_constraint(v, pltpu.VMEM) for v in (h, acc, u, wd))
    new_up, new_dn, y, _, _ = pl.pallas_call(
        last_kernel,
        out_shape=(
            jax.ShapeDtypeStruct(up_shape, jnp.float32),
            jax.ShapeDtypeStruct(dn_shape, jnp.float32),
            jax.ShapeDtypeStruct(y_shape, jnp.bfloat16),
            pltpu.VMEM((TOKENS, DIM), jnp.bfloat16),
            pltpu.VMEM((TOKENS, DIM), jnp.float32),
        ),
        in_specs=[pl.BlockSpec(memory_space=pltpu.SMEM), hbm] + [vmem] * 4,
        out_specs=(hbm, hbm, hbm, vmem, vmem),
        input_output_aliases={2: 3, 3: 4},
        scratch_shapes=[
            pltpu.VMEM((PART_ROWS, CHUNK), jnp.float32),
            dma, dma, dma((BACK,)), dma((BACK,)), dma,
        ],
        compiler_params=pltpu.CompilerParams(vmem_limit_bytes=STACK_VMEM),
        cost_estimate=pl.CostEstimate(flops=18_000_000_000, bytes_accessed=67_000_000, transcendentals=2_000_000),
        name="last",
    )(lens, left, h, acc, u, wd)
    return new_up, new_dn, y


def solution(mesh):
    up_spec = P("side", None, "rep", None)
    down_spec = P("side", None, None, "rep")
    act_spec = P("side", "rep", None)

    def device_step(w_up, w_down, g_up, g_down, learn_rate, prompts, prompt_lens):
        _, left, h, acc, u, _, wd = mlp_stack(
            learn_rate.reshape(1), prompt_lens, w_up, g_up, w_down, g_down, prompts[0]
        )
        return last_step(prompt_lens, left, h, acc, u, wd, w_up.shape, w_down.shape, prompts.shape)

    return jax.shard_map(
        device_step,
        mesh=mesh,
        in_specs=(up_spec, down_spec, up_spec, down_spec, P(), act_spec, P("rep")),
        out_specs=(up_spec, down_spec, act_spec),
        check_vma=False,
    )
```

```python
import jax
import jax.numpy as jnp
from jax import lax
from jax.experimental import pallas as pl
from jax.experimental.pallas import tpu as pltpu
from jax.sharding import PartitionSpec as P

MESH = pl.DeviceIdType.MESH
LAYERS, DIM, FFN, TOKENS = 2, 2048, 6144, 4096
RANKS = 4
COLS = DIM // RANKS
CHUNK = 512
CHUNKS = LAYERS * FFN // CHUNK
PER_LAYER = FFN // CHUNK
PARTS = 4
PART_ROWS = 2 * CHUNK // PARTS
PIECES = CHUNKS * PARTS
BLOCK = 256
TILE = 1024
TILES = TOKENS // TILE
PHASE = TILES
LAST = CHUNKS - 1
STEPS = LAST * 2 * PHASE + PHASE
AHEAD, X_LAG, PAIR_LAG = 7, 3, 1
PER = 2 * PHASE // PARTS
WINDOW = 4
RING = 8
STAGES = 3
HELD = 56
BACK = 8
OUT_TILE = 512
BLOCKS = TOKENS // BLOCK
GROUP = 64
STACK_VMEM = 8_300_000


def gelu(z):
    return 0.5 * z * (1.0 + jnp.tanh(0.7978845608 * (z + 0.044715 * (z * z * z))))


def piece_of(up_ref, dn_ref, c, k):
    layer, col = c // PER_LAYER, lax.rem(c, PER_LAYER) * CHUNK
    if k < PARTS // 2:
        cols = pl.ds(pl.multiple_of(col, CHUNK), CHUNK)
        return up_ref.at[0, layer, pl.ds(k * PART_ROWS, PART_ROWS), cols]
    first = pl.multiple_of(col + (k - PARTS // 2) * PART_ROWS, PART_ROWS)
    return dn_ref.at[0, layer, pl.ds(first, PART_ROWS), :]


def held_piece(acc, c, k):
    return acc.at[pl.ds(pl.multiple_of(c * PART_ROWS, PART_ROWS), PART_ROWS), pl.ds(k * CHUNK, CHUNK)]


def stage(acc, s):
    first = pl.multiple_of((HELD + s) // PARTS * PART_ROWS, PART_ROWS)
    col = pl.multiple_of(lax.rem(s, PARTS) * CHUNK, CHUNK)
    return acc.at[pl.ds(first, PART_ROWS), pl.ds(col, CHUNK)]


def block_rows(b):
    return pl.ds(pl.multiple_of(b * BLOCK, BLOCK), BLOCK)


def down_cols(n):
    return slice(n * COLS, (n + 1) * COLS)


def down(u, wd, b, n):
    return jnp.dot(u[b], wd[n].reshape(CHUNK, COLS), preferred_element_type=jnp.float32)


def stack_kernel(
    lr_ref, lens, w_up, g_up, w_dn, g_dn, x_ref, land, left, h, acc, u, wu, wd,
    pre, y_send, y_recv, x_send, x_recv, own_send, own_recv, far_send, far_recv,
    w_sem, x_sem, w_in, g_in, left_sem,
):
    del lens
    side, rep = lax.axis_index("side"), lax.axis_index("rep")
    pair = rep + 1 - 2 * lax.rem(rep, 2)
    cross = lax.rem(rep + 2, RANKS)
    cross_pair = lax.rem(pair + 2, RANKS)

    def remote(src, piece, slot, send, recv, to):
        return pltpu.make_async_remote_copy(
            src_ref=src, dst_ref=land.at[piece, slot], send_sem=send, recv_sem=recv,
            device_id=to, device_id_type=MESH,
        )

    def y_copy(p):
        return remote(u.at[lax.rem(p, RING)], p, rep, y_send.at[lax.rem(p, WINDOW)], y_recv.at[p], (1, rep))

    def x_copy(p, slot):
        return remote(land.at[p, slot], p, slot, x_send.at[lax.rem(p, RING)], x_recv.at[p], (1, cross))

    def own_copy(p, slot):
        return remote(land.at[p, slot], p, slot, own_send.at[lax.rem(p, RING)], own_recv.at[p], (1, pair))

    def far_copy(p, slot):
        return remote(land.at[p, slot], p, slot, far_send.at[lax.rem(p, RING)], far_recv.at[p], (1, pair))

    def load(p, k):
        half = PARTS // 2
        to = wu.at[:, k] if k < half else wd.at[:, k - half]
        return pltpu.make_async_copy(land.at[p], to, w_sem.at[k])

    barrier = pltpu.get_barrier_semaphore()

    @pl.when(side == 0)
    def trainer():
        def w_stage(s):
            return stage(acc, s)

        def g_stage(s):
            return stage(acc, PARTS + s)

        def fetch(c, k):
            s = lax.rem(c * PARTS + k, STAGES)
            return (
                pltpu.make_async_copy(piece_of(w_up, w_dn, c, k), w_stage(s), w_in.at[s]),
                pltpu.make_async_copy(piece_of(g_up, g_dn, c, k), g_stage(s), g_in.at[s]),
            )

        def spill(p):
            s = lax.rem(p, STAGES)
            return pltpu.make_async_copy(w_stage(s), left.at[p - HELD], left_sem.at[s])

        for k in range(2):
            for copy in fetch(0, k):
                copy.start()
        pl.semaphore_signal(barrier, inc=1, device_id=(1, rep), device_id_type=MESH)
        pl.semaphore_wait(barrier, 1)
        lr = lr_ref[0]

        def send(p):
            @pl.when(p >= WINDOW)
            def _():
                y_copy(p - WINDOW).wait_send()

            y_copy(p).start()

        def chunk(c, _):
            for k in range(PARTS):
                p = c * PARTS + k
                for copy in fetch(c, k):
                    copy.wait()
                s = lax.rem(p, STAGES)
                new = w_stage(s)[...] - lr * g_stage(s)[...]
                u[lax.rem(p, RING)] = new.astype(jnp.bfloat16)

                @pl.when(p < HELD)
                def _():
                    held_piece(acc, c, k)[...] = new

                @pl.when(p >= HELD)
                def _():
                    w_stage(s)[...] = new

                @pl.when(p >= 1)
                def _():
                    send(p - 1)

                @pl.when(p - 1 >= HELD)
                def _():
                    spill(p - 1).start()
                    spill(p - 1).wait()

                ahead = k + 2

                @pl.when(p + 2 < PIECES)
                def _():
                    for copy in fetch(c + ahead // PARTS, ahead % PARTS):
                        copy.start()

            return 0

        lax.fori_loop(0, CHUNKS, chunk, 0)
        send(PIECES - 1)
        spill(PIECES - 1).start()
        spill(PIECES - 1).wait()

        def drain(p, _):
            y_copy(p).wait_send()
            return 0

        lax.fori_loop(PIECES - WINDOW, PIECES, drain, 0)

    @pl.when(side == 1)
    def generator():
        x_in = pltpu.make_async_copy(x_ref, h, x_sem)
        x_in.start()
        pre[...] = jnp.zeros_like(pre)
        for to in ((0, rep), (1, pair), (1, cross)):
            pl.semaphore_signal(barrier, inc=1, device_id=to, device_id_type=MESH)
        pl.semaphore_wait(barrier, 3)

        def event(s, lag, fn):
            q = s + AHEAD - lag
            p = q // PER
            pl.when((lax.rem(q + PER * PIECES, PER) == 0) & (p >= 0) & (p < PIECES))(lambda: fn(p))

        def on_y(p):
            y_copy(p).wait_recv()

            @pl.when(p >= RING)
            def _():
                x_copy(p - RING, rep).wait_send()
                own_copy(p - RING, rep).wait_send()

            x_copy(p, rep).start()
            own_copy(p, rep).start()

        def on_x(p):
            x_copy(p, cross).wait_recv()

            @pl.when(p >= RING)
            def _():
                far_copy(p - RING, cross).wait_send()

            far_copy(p, cross).start()

        def on_pair(p):
            own_copy(p, pair).wait_recv()
            far_copy(p, cross_pair).wait_recv()
            for k in range(PARTS):
                pl.when(lax.rem(p, PARTS) == k)(lambda k=k: load(p, k).start())

        def up_phase(c, i):
            @pl.when(i == 0)
            def _():
                for k in range(PARTS // 2):
                    load(c * PARTS + k, k).wait()

            for j in range(TILE // BLOCK):
                b = i * (TILE // BLOCK) + j
                z = jnp.dot(h[block_rows(b), :], wu[...].reshape(DIM, CHUNK), preferred_element_type=jnp.float32)
                act_of_pre(lax.rem(b + BLOCKS - 1, BLOCKS))
                pre[...] = z

        def act_of_pre(b):
            u[b] = gelu(pre[...]).astype(jnp.bfloat16)

        def last_act():
            def group(q, _):
                rows = pl.ds(pl.multiple_of(q * GROUP, GROUP), GROUP)
                u[BLOCKS - 1, rows, :] = gelu(pre[rows, :]).astype(jnp.bfloat16)
                return 0

            lax.fori_loop(0, BLOCK // GROUP, group, 0)

        def down_phase(c, i):
            @pl.when(i == 0)
            def _():
                last_act()
                for k in range(PARTS // 2, PARTS):
                    load(c * PARTS + k, k).wait()

            for j in range(TILE // BLOCK):
                b = i * (TILE // BLOCK) + j
                for n in range(RANKS):
                    acc[block_rows(b), down_cols(n)] += down(u, wd, b, n)

            @pl.when(lax.rem(c, PER_LAYER) == PER_LAYER - 1)
            def _():
                lax.fori_loop(0, TILE // BLOCK, lambda j, _: next_h(i * (TILE // BLOCK) + j), 0)

        def next_h(b):
            h[block_rows(b), :] = acc[block_rows(b), :].astype(jnp.bfloat16)
            acc[block_rows(b), :] = h[block_rows(b), :].astype(jnp.float32)
            return 0

        def first_acc(b):
            acc[block_rows(b), :] = h[block_rows(b), :].astype(jnp.float32)
            return 0

        def step(t, _):
            s = t - AHEAD
            event(s, 0, on_y)
            event(s, X_LAG, on_x)
            event(s, X_LAG + PAIR_LAG, on_pair)

            @pl.when((s < 0) & (s >= -TILES))
            def _():
                i = s + TILES

                @pl.when(i == 0)
                def _():
                    x_in.wait()

                lax.fori_loop(0, TILE // BLOCK, lambda j, _: first_acc(i * (TILE // BLOCK) + j), 0)

            c, i = s // (2 * PHASE), lax.rem(s + 2 * PHASE, 2 * PHASE)

            @pl.when((s >= 0) & (i < PHASE))
            def _():
                up_phase(c, i)

            @pl.when((s >= 0) & (i >= PHASE))
            def _():
                down_phase(c, i - PHASE)

            return 0

        lax.fori_loop(0, AHEAD + STEPS, step, 0)
        last_act()

        def drain(p, _):
            x_copy(p, rep).wait_send()
            own_copy(p, rep).wait_send()
            far_copy(p, cross).wait_send()
            return 0

        lax.fori_loop(PIECES - RING, PIECES, drain, 0)
        for k in range(PARTS // 2, PARTS):
            load(LAST * PARTS + k, k).wait()


def mlp_stack(lr, lens, w_up, g_up, w_dn, g_dn, x):
    dma = pltpu.SemaphoreType.DMA
    hbm = pl.BlockSpec(memory_space=pl.ANY)
    vmem = pl.BlockSpec(memory_space=pltpu.VMEM)
    return pl.pallas_call(
        stack_kernel,
        out_shape=(
            jax.ShapeDtypeStruct((PIECES, RANKS, PART_ROWS, CHUNK), jnp.bfloat16),
            jax.ShapeDtypeStruct((PIECES - HELD, PART_ROWS, CHUNK), jnp.float32),
            pltpu.VMEM((TOKENS, DIM), jnp.bfloat16),
            pltpu.VMEM((TOKENS, DIM), jnp.float32),
            pltpu.VMEM((TOKENS // BLOCK, BLOCK, CHUNK), jnp.bfloat16),
            pltpu.VMEM((RANKS, PARTS // 2, PART_ROWS, CHUNK), jnp.bfloat16),
            pltpu.VMEM((RANKS, PARTS // 2, PART_ROWS, COLS), jnp.bfloat16),
        ),
        in_specs=[pl.BlockSpec(memory_space=pltpu.SMEM)] * 2 + [hbm] * 5,
        out_specs=(hbm, hbm) + (vmem,) * 5,
        scratch_shapes=[
            pltpu.VMEM((BLOCK, CHUNK), jnp.float32),
            dma((WINDOW,)), dma((PIECES,)),
            dma((RING,)), dma((PIECES,)),
            dma((RING,)), dma((PIECES,)),
            dma((RING,)), dma((PIECES,)),
            dma((PARTS,)), dma, dma((STAGES,)), dma((STAGES,)), dma((STAGES,)),
        ],
        compiler_params=pltpu.CompilerParams(
            collective_id=0, has_side_effects=True, vmem_limit_bytes=STACK_VMEM
        ),
        cost_estimate=pl.CostEstimate(flops=400_000_000_000, bytes_accessed=300_000_000, transcendentals=50_000_000),
        name="stack",
    )(lr, lens, w_up, g_up, w_dn, g_dn, x)


def last_kernel(
    lens, left, h_in, acc_in, u, wd, new_up, new_dn, y_ref, h, acc, zero,
    zero_sem, held_sem, back_in, back_out, y_sem,
):
    del h_in
    side = lax.axis_index("side")

    def y_copy(src, b):
        return pltpu.make_async_copy(h.at[block_rows(src)], y_ref.at[0, block_rows(b)], y_sem)

    @pl.when(side == 0)
    def trainer():
        def held_copy(c, k):
            return pltpu.make_async_copy(held_piece(acc_in, c, k), piece_of(new_up, new_dn, c, k), held_sem)

        def each(lo, hi, fn):
            def body(c, _):
                for k in range(PARTS):
                    fn(c, k)
                return 0

            lax.fori_loop(lo, hi, body, 0)

        def back_read(c, k):
            b = lax.rem(c, BACK // PARTS) * PARTS + k
            return pltpu.make_async_copy(left.at[c * PARTS + k - HELD], stage(acc, b), back_in.at[b])

        def back_write(c, k):
            b = lax.rem(c, BACK // PARTS) * PARTS + k
            return pltpu.make_async_copy(stage(acc, b), piece_of(new_up, new_dn, c, k), back_out.at[b])

        held, blocks = HELD // PARTS, TOKENS // BLOCK
        each(held, held + BACK // PARTS, lambda c, k: back_read(c, k).start())
        h[block_rows(0), :] = jnp.zeros((BLOCK, DIM), jnp.bfloat16)

        def bring(c, _):
            for a in (c - held, c - held + CHUNKS - held):
                @pl.when(a < held)
                def _():
                    for k in range(PARTS):
                        held_copy(a, k).start()

            for k in range(PARTS):
                back_read(c, k).wait()
                back_write(c, k).start()

            @pl.when((c > held) & (c + 1 < CHUNKS))
            def _():
                for k in range(PARTS):
                    back_write(c - 1, k).wait()
                    back_read(c + 1, k).start()

            for b in (2 * (c - held), 2 * (c - held) + 1):
                @pl.when(b < blocks)
                def _():
                    y_copy(0, b).start()

            return 0

        lax.fori_loop(held, CHUNKS, bring, 0)
        each(0, held, lambda c, k: held_copy(c, k).wait())
        each(CHUNKS - 2, CHUNKS, lambda c, k: back_write(c, k).wait())
        for b in range(blocks):
            y_copy(0, b).wait()

    @pl.when(side == 1)
    def generator():
        zero[...] = jnp.zeros_like(zero)

        def each_zero(fn):
            def body(c, _):
                for k in range(PARTS):
                    fn(pltpu.make_async_copy(zero, piece_of(new_up, new_dn, c, k), zero_sem))
                return 0

            lax.fori_loop(0, CHUNKS, body, 0)

        each_zero(lambda copy: copy.start())
        length = lens[0]
        per = OUT_TILE // BLOCK

        def send(i):
            for j in range(per):
                y_copy(i * per + j, i * per + j).start()

        def step(i, _):
            for j in range(per):
                b = i * per + j
                at = lax.broadcasted_iota(jnp.int32, (BLOCK, COLS), 0) + b * BLOCK
                for n in range(RANKS):
                    total = acc_in[block_rows(b), down_cols(n)] + down(u, wd, b, n)
                    h[block_rows(b), down_cols(n)] = jnp.where(at < length, total, 0.0).astype(jnp.bfloat16)

            pl.when(i >= 1)(lambda: send(i - 1))
            return 0

        steps = TOKENS // OUT_TILE
        lax.fori_loop(0, steps, step, 0)
        send(steps - 1)
        each_zero(lambda copy: copy.wait())
        for b in range(TOKENS // BLOCK):
            y_copy(b, b).wait()


def last_step(lens, left, h, acc, u, wd, up_shape, dn_shape, y_shape):
    dma = pltpu.SemaphoreType.DMA
    hbm = pl.BlockSpec(memory_space=pl.ANY)
    vmem = pl.BlockSpec(memory_space=pltpu.VMEM)
    h, acc, u, wd = (pltpu.with_memory_space_constraint(v, pltpu.VMEM) for v in (h, acc, u, wd))
    new_up, new_dn, y, _, _ = pl.pallas_call(
        last_kernel,
        out_shape=(
            jax.ShapeDtypeStruct(up_shape, jnp.float32),
            jax.ShapeDtypeStruct(dn_shape, jnp.float32),
            jax.ShapeDtypeStruct(y_shape, jnp.bfloat16),
            pltpu.VMEM((TOKENS, DIM), jnp.bfloat16),
            pltpu.VMEM((TOKENS, DIM), jnp.float32),
        ),
        in_specs=[pl.BlockSpec(memory_space=pltpu.SMEM), hbm] + [vmem] * 4,
        out_specs=(hbm, hbm, hbm, vmem, vmem),
        input_output_aliases={2: 3, 3: 4},
        scratch_shapes=[
            pltpu.VMEM((PART_ROWS, CHUNK), jnp.float32),
            dma, dma, dma((BACK,)), dma((BACK,)), dma,
        ],
        compiler_params=pltpu.CompilerParams(vmem_limit_bytes=STACK_VMEM),
        cost_estimate=pl.CostEstimate(flops=18_000_000_000, bytes_accessed=67_000_000, transcendentals=2_000_000),
        name="last",
    )(lens, left, h, acc, u, wd)
    return new_up, new_dn, y


def solution(mesh):
    up_spec = P("side", None, "rep", None)
    down_spec = P("side", None, None, "rep")
    act_spec = P("side", "rep", None)

    def device_step(w_up, w_down, g_up, g_down, learn_rate, prompts, prompt_lens):
        _, left, h, acc, u, _, wd = mlp_stack(
            learn_rate.reshape(1), prompt_lens, w_up, g_up, w_down, g_down, prompts[0]
        )
        return last_step(prompt_lens, left, h, acc, u, wd, w_up.shape, w_down.shape, prompts.shape)

    return jax.shard_map(
        device_step,
        mesh=mesh,
        in_specs=(up_spec, down_spec, up_spec, down_spec, P(), act_spec, P("rep")),
        out_specs=(up_spec, down_spec, act_spec),
        check_vma=False,
    )
```

```python
import jax
import jax.numpy as jnp
from jax import lax
from jax.experimental import pallas as pl
from jax.experimental.pallas import tpu as pltpu
from jax.sharding import PartitionSpec as P

MESH = pl.DeviceIdType.MESH
LAYERS, DIM, FFN, TOKENS = 2, 2048, 6144, 4096
RANKS = 4
COLS = DIM // RANKS
CHUNK = 512
CHUNKS = LAYERS * FFN // CHUNK
PER_LAYER = FFN // CHUNK
PARTS = 8
PART_ROWS = 2 * CHUNK // PARTS
PIECES = CHUNKS * PARTS
BLOCK = 256
TILE = 1024
TILES = TOKENS // TILE
PHASE = TILES
LAST = CHUNKS - 1
STEPS = LAST * 2 * PHASE + PHASE
AHEAD, X_LAG, PAIR_LAG = 7, 2, 1
PER = 2 * PHASE // PARTS
WINDOW = 4
RING = 8
STAGES = 3
HELD = 112
BACK = 16
OUT_TILE = 512
BLOCKS = TOKENS // BLOCK
GROUP = 64
STACK_VMEM = 8_300_000


def gelu(z):
    return 0.5 * z * (1.0 + jnp.tanh(0.7978845608 * (z + 0.044715 * (z * z * z))))


def piece_of(up_ref, dn_ref, c, k):
    layer, col = c // PER_LAYER, lax.rem(c, PER_LAYER) * CHUNK
    if k < PARTS // 2:
        cols = pl.ds(pl.multiple_of(col, CHUNK), CHUNK)
        return up_ref.at[0, layer, pl.ds(k * PART_ROWS, PART_ROWS), cols]
    first = pl.multiple_of(col + (k - PARTS // 2) * PART_ROWS, PART_ROWS)
    return dn_ref.at[0, layer, pl.ds(first, PART_ROWS), :]


ACROSS = DIM // CHUNK


def held_piece(acc, c, k):
    first = pl.multiple_of((c * (PARTS // ACROSS) + k // ACROSS) * PART_ROWS, PART_ROWS)
    return acc.at[pl.ds(first, PART_ROWS), pl.ds(k % ACROSS * CHUNK, CHUNK)]


def stage(acc, s):
    first = pl.multiple_of((HELD + s) // ACROSS * PART_ROWS, PART_ROWS)
    col = pl.multiple_of(lax.rem(s, ACROSS) * CHUNK, CHUNK)
    return acc.at[pl.ds(first, PART_ROWS), pl.ds(col, CHUNK)]


def block_rows(b):
    return pl.ds(pl.multiple_of(b * BLOCK, BLOCK), BLOCK)


def down_cols(n):
    return slice(n * COLS, (n + 1) * COLS)


def down(u, wd, b, n):
    return jnp.dot(u[b], wd[n].reshape(CHUNK, COLS), preferred_element_type=jnp.float32)


def stack_kernel(
    lr_ref, lens, w_up, g_up, w_dn, g_dn, x_ref, land, left, h, acc, u, wu, wd,
    pre, y_send, y_recv, x_send, x_recv, own_send, own_recv, far_send, far_recv,
    w_sem, x_sem, w_in, g_in, left_sem,
):
    del lens
    side, rep = lax.axis_index("side"), lax.axis_index("rep")
    pair = rep + 1 - 2 * lax.rem(rep, 2)
    cross = lax.rem(rep + 2, RANKS)
    cross_pair = lax.rem(pair + 2, RANKS)

    def remote(src, piece, slot, send, recv, to):
        return pltpu.make_async_remote_copy(
            src_ref=src, dst_ref=land.at[piece, slot], send_sem=send, recv_sem=recv,
            device_id=to, device_id_type=MESH,
        )

    def y_copy(p):
        return remote(u.at[lax.rem(p, RING), pl.ds(0, PART_ROWS)], p, rep, y_send.at[lax.rem(p, WINDOW)], y_recv.at[p], (1, rep))

    def x_copy(p, slot):
        return remote(land.at[p, slot], p, slot, x_send.at[lax.rem(p, RING)], x_recv.at[p], (1, cross))

    def own_copy(p, slot):
        return remote(land.at[p, slot], p, slot, own_send.at[lax.rem(p, RING)], own_recv.at[p], (1, pair))

    def far_copy(p, slot):
        return remote(land.at[p, slot], p, slot, far_send.at[lax.rem(p, RING)], far_recv.at[p], (1, pair))

    def load(p, k):
        half = PARTS // 2
        to = wu.at[:, k] if k < half else wd.at[:, k - half]
        return pltpu.make_async_copy(land.at[p], to, w_sem.at[k])

    barrier = pltpu.get_barrier_semaphore()

    @pl.when(side == 0)
    def trainer():
        def w_stage(s):
            return stage(acc, s)

        def g_stage(s):
            return stage(acc, PARTS + s)

        def fetch(c, k):
            s = lax.rem(c * PARTS + k, STAGES)
            return (
                pltpu.make_async_copy(piece_of(w_up, w_dn, c, k), w_stage(s), w_in.at[s]),
                pltpu.make_async_copy(piece_of(g_up, g_dn, c, k), g_stage(s), g_in.at[s]),
            )

        def spill(p):
            s = lax.rem(p, STAGES)
            return pltpu.make_async_copy(w_stage(s), left.at[p - HELD], left_sem.at[s])

        for k in range(2):
            for copy in fetch(0, k):
                copy.start()
        pl.semaphore_signal(barrier, inc=1, device_id=(1, rep), device_id_type=MESH)
        pl.semaphore_wait(barrier, 1)
        lr = lr_ref[0]

        def send(p):
            @pl.when(p >= WINDOW)
            def _():
                y_copy(p - WINDOW).wait_send()

            y_copy(p).start()

        def chunk(c, _):
            for k in range(PARTS):
                p = c * PARTS + k
                for copy in fetch(c, k):
                    copy.wait()
                s = lax.rem(p, STAGES)
                new = w_stage(s)[...] - lr * g_stage(s)[...]
                u[lax.rem(p, RING), 0:PART_ROWS, :] = new.astype(jnp.bfloat16)

                @pl.when(p < HELD)
                def _():
                    held_piece(acc, c, k)[...] = new

                @pl.when(p >= HELD)
                def _():
                    w_stage(s)[...] = new

                @pl.when(p >= 1)
                def _():
                    send(p - 1)

                @pl.when(p - 1 >= HELD)
                def _():
                    spill(p - 1).start()
                    spill(p - 1).wait()

                ahead = k + 2

                @pl.when(p + 2 < PIECES)
                def _():
                    for copy in fetch(c + ahead // PARTS, ahead % PARTS):
                        copy.start()

            return 0

        lax.fori_loop(0, CHUNKS, chunk, 0)
        send(PIECES - 1)
        spill(PIECES - 1).start()
        spill(PIECES - 1).wait()

        def drain(p, _):
            y_copy(p).wait_send()
            return 0

        lax.fori_loop(PIECES - WINDOW, PIECES, drain, 0)

    @pl.when(side == 1)
    def generator():
        x_in = pltpu.make_async_copy(x_ref, h, x_sem)
        x_in.start()
        pre[...] = jnp.zeros_like(pre)
        for to in ((0, rep), (1, pair), (1, cross)):
            pl.semaphore_signal(barrier, inc=1, device_id=to, device_id_type=MESH)
        pl.semaphore_wait(barrier, 3)

        def event(s, lag, fn):
            q = s + AHEAD - lag
            p = q // PER
            pl.when((lax.rem(q + PER * PIECES, PER) == 0) & (p >= 0) & (p < PIECES))(lambda: fn(p))

        def on_y(p):
            y_copy(p).wait_recv()

            @pl.when(p >= RING)
            def _():
                x_copy(p - RING, rep).wait_send()
                own_copy(p - RING, rep).wait_send()

            x_copy(p, rep).start()
            own_copy(p, rep).start()

        def on_x(p):
            x_copy(p, cross).wait_recv()

            @pl.when(p >= RING)
            def _():
                far_copy(p - RING, cross).wait_send()

            far_copy(p, cross).start()

        def on_pair(p):
            own_copy(p, pair).wait_recv()
            far_copy(p, cross_pair).wait_recv()
            for k in range(PARTS):
                pl.when(lax.rem(p, PARTS) == k)(lambda k=k: load(p, k).start())

        def up_phase(c, i):
            @pl.when(i == 0)
            def _():
                for k in range(PARTS // 2):
                    load(c * PARTS + k, k).wait()

            for j in range(TILE // BLOCK):
                b = i * (TILE // BLOCK) + j
                z = jnp.dot(h[block_rows(b), :], wu[...].reshape(DIM, CHUNK), preferred_element_type=jnp.float32)
                act_of_pre(lax.rem(b + BLOCKS - 1, BLOCKS))
                pre[...] = z

        def act_of_pre(b):
            u[b] = gelu(pre[...]).astype(jnp.bfloat16)

        def last_act():
            def group(q, _):
                rows = pl.ds(pl.multiple_of(q * GROUP, GROUP), GROUP)
                u[BLOCKS - 1, rows, :] = gelu(pre[rows, :]).astype(jnp.bfloat16)
                return 0

            lax.fori_loop(0, BLOCK // GROUP, group, 0)

        def down_phase(c, i):
            @pl.when(i == 0)
            def _():
                last_act()
                for k in range(PARTS // 2, PARTS):
                    load(c * PARTS + k, k).wait()

            for j in range(TILE // BLOCK):
                b = i * (TILE // BLOCK) + j
                for n in range(RANKS):
                    acc[block_rows(b), down_cols(n)] += down(u, wd, b, n)

            @pl.when(lax.rem(c, PER_LAYER) == PER_LAYER - 1)
            def _():
                lax.fori_loop(0, TILE // BLOCK, lambda j, _: next_h(i * (TILE // BLOCK) + j), 0)

        def next_h(b):
            h[block_rows(b), :] = acc[block_rows(b), :].astype(jnp.bfloat16)
            acc[block_rows(b), :] = h[block_rows(b), :].astype(jnp.float32)
            return 0

        def first_acc(b):
            acc[block_rows(b), :] = h[block_rows(b), :].astype(jnp.float32)
            return 0

        def step(t, _):
            s = t - AHEAD
            event(s, 0, on_y)
            event(s, X_LAG, on_x)
            event(s, X_LAG + PAIR_LAG, on_pair)

            @pl.when((s < 0) & (s >= -TILES))
            def _():
                i = s + TILES

                @pl.when(i == 0)
                def _():
                    x_in.wait()

                lax.fori_loop(0, TILE // BLOCK, lambda j, _: first_acc(i * (TILE // BLOCK) + j), 0)

            c, i = s // (2 * PHASE), lax.rem(s + 2 * PHASE, 2 * PHASE)

            @pl.when((s >= 0) & (i < PHASE))
            def _():
                up_phase(c, i)

            @pl.when((s >= 0) & (i >= PHASE))
            def _():
                down_phase(c, i - PHASE)

            return 0

        lax.fori_loop(0, AHEAD + STEPS, step, 0)
        last_act()

        def drain(p, _):
            x_copy(p, rep).wait_send()
            own_copy(p, rep).wait_send()
            far_copy(p, cross).wait_send()
            return 0

        lax.fori_loop(PIECES - RING, PIECES, drain, 0)
        for k in range(PARTS // 2, PARTS):
            load(LAST * PARTS + k, k).wait()


def mlp_stack(lr, lens, w_up, g_up, w_dn, g_dn, x):
    dma = pltpu.SemaphoreType.DMA
    hbm = pl.BlockSpec(memory_space=pl.ANY)
    vmem = pl.BlockSpec(memory_space=pltpu.VMEM)
    return pl.pallas_call(
        stack_kernel,
        out_shape=(
            jax.ShapeDtypeStruct((PIECES, RANKS, PART_ROWS, CHUNK), jnp.bfloat16),
            jax.ShapeDtypeStruct((PIECES - HELD, PART_ROWS, CHUNK), jnp.float32),
            pltpu.VMEM((TOKENS, DIM), jnp.bfloat16),
            pltpu.VMEM((TOKENS, DIM), jnp.float32),
            pltpu.VMEM((TOKENS // BLOCK, BLOCK, CHUNK), jnp.bfloat16),
            pltpu.VMEM((RANKS, PARTS // 2, PART_ROWS, CHUNK), jnp.bfloat16),
            pltpu.VMEM((RANKS, PARTS // 2, PART_ROWS, COLS), jnp.bfloat16),
        ),
        in_specs=[pl.BlockSpec(memory_space=pltpu.SMEM)] * 2 + [hbm] * 5,
        out_specs=(hbm, hbm) + (vmem,) * 5,
        scratch_shapes=[
            pltpu.VMEM((BLOCK, CHUNK), jnp.float32),
            dma((WINDOW,)), dma((PIECES,)),
            dma((RING,)), dma((PIECES,)),
            dma((RING,)), dma((PIECES,)),
            dma((RING,)), dma((PIECES,)),
            dma((PARTS,)), dma, dma((STAGES,)), dma((STAGES,)), dma((STAGES,)),
        ],
        compiler_params=pltpu.CompilerParams(
            collective_id=0, has_side_effects=True, vmem_limit_bytes=STACK_VMEM
        ),
        cost_estimate=pl.CostEstimate(flops=400_000_000_000, bytes_accessed=300_000_000, transcendentals=50_000_000),
        name="stack",
    )(lr, lens, w_up, g_up, w_dn, g_dn, x)


def last_kernel(
    lens, left, h_in, acc_in, u, wd, new_up, new_dn, y_ref, h, acc, zero,
    zero_sem, held_sem, back_in, back_out, y_sem,
):
    del h_in
    side = lax.axis_index("side")

    def y_copy(src, b):
        return pltpu.make_async_copy(h.at[block_rows(src)], y_ref.at[0, block_rows(b)], y_sem)

    @pl.when(side == 0)
    def trainer():
        def held_copy(c, k):
            return pltpu.make_async_copy(held_piece(acc_in, c, k), piece_of(new_up, new_dn, c, k), held_sem)

        def each(lo, hi, fn):
            def body(c, _):
                for k in range(PARTS):
                    fn(c, k)
                return 0

            lax.fori_loop(lo, hi, body, 0)

        def back_read(c, k):
            b = lax.rem(c, BACK // PARTS) * PARTS + k
            return pltpu.make_async_copy(left.at[c * PARTS + k - HELD], stage(acc, b), back_in.at[b])

        def back_write(c, k):
            b = lax.rem(c, BACK // PARTS) * PARTS + k
            return pltpu.make_async_copy(stage(acc, b), piece_of(new_up, new_dn, c, k), back_out.at[b])

        held, blocks = HELD // PARTS, TOKENS // BLOCK
        each(held, held + BACK // PARTS, lambda c, k: back_read(c, k).start())
        h[block_rows(0), :] = jnp.zeros((BLOCK, DIM), jnp.bfloat16)

        def bring(c, _):
            for a in (c - held, c - held + CHUNKS - held):
                @pl.when(a < held)
                def _():
                    for k in range(PARTS):
                        held_copy(a, k).start()

            for k in range(PARTS):
                back_read(c, k).wait()
                back_write(c, k).start()

            @pl.when((c > held) & (c + 1 < CHUNKS))
            def _():
                for k in range(PARTS):
                    back_write(c - 1, k).wait()
                    back_read(c + 1, k).start()

            for b in (2 * (c - held), 2 * (c - held) + 1):
                @pl.when(b < blocks)
                def _():
                    y_copy(0, b).start()

            return 0

        lax.fori_loop(held, CHUNKS, bring, 0)
        each(0, held, lambda c, k: held_copy(c, k).wait())
        each(CHUNKS - 2, CHUNKS, lambda c, k: back_write(c, k).wait())
        for b in range(blocks):
            y_copy(0, b).wait()

    @pl.when(side == 1)
    def generator():
        zero[...] = jnp.zeros_like(zero)

        def each_zero(fn):
            def body(c, _):
                for k in range(PARTS):
                    fn(pltpu.make_async_copy(zero, piece_of(new_up, new_dn, c, k), zero_sem))
                return 0

            lax.fori_loop(0, CHUNKS, body, 0)

        each_zero(lambda copy: copy.start())
        length = lens[0]
        per = OUT_TILE // BLOCK

        def send(i):
            for j in range(per):
                y_copy(i * per + j, i * per + j).start()

        def step(i, _):
            for j in range(per):
                b = i * per + j
                at = lax.broadcasted_iota(jnp.int32, (BLOCK, COLS), 0) + b * BLOCK
                for n in range(RANKS):
                    total = acc_in[block_rows(b), down_cols(n)] + down(u, wd, b, n)
                    h[block_rows(b), down_cols(n)] = jnp.where(at < length, total, 0.0).astype(jnp.bfloat16)

            pl.when(i >= 1)(lambda: send(i - 1))
            return 0

        steps = TOKENS // OUT_TILE
        lax.fori_loop(0, steps, step, 0)
        send(steps - 1)
        each_zero(lambda copy: copy.wait())
        for b in range(TOKENS // BLOCK):
            y_copy(b, b).wait()


def last_step(lens, left, h, acc, u, wd, up_shape, dn_shape, y_shape):
    dma = pltpu.SemaphoreType.DMA
    hbm = pl.BlockSpec(memory_space=pl.ANY)
    vmem = pl.BlockSpec(memory_space=pltpu.VMEM)
    h, acc, u, wd = (pltpu.with_memory_space_constraint(v, pltpu.VMEM) for v in (h, acc, u, wd))
    new_up, new_dn, y, _, _ = pl.pallas_call(
        last_kernel,
        out_shape=(
            jax.ShapeDtypeStruct(up_shape, jnp.float32),
            jax.ShapeDtypeStruct(dn_shape, jnp.float32),
            jax.ShapeDtypeStruct(y_shape, jnp.bfloat16),
            pltpu.VMEM((TOKENS, DIM), jnp.bfloat16),
            pltpu.VMEM((TOKENS, DIM), jnp.float32),
        ),
        in_specs=[pl.BlockSpec(memory_space=pltpu.SMEM), hbm] + [vmem] * 4,
        out_specs=(hbm, hbm, hbm, vmem, vmem),
        input_output_aliases={2: 3, 3: 4},
        scratch_shapes=[
            pltpu.VMEM((PART_ROWS, CHUNK), jnp.float32),
            dma, dma, dma((BACK,)), dma((BACK,)), dma,
        ],
        compiler_params=pltpu.CompilerParams(vmem_limit_bytes=STACK_VMEM),
        cost_estimate=pl.CostEstimate(flops=18_000_000_000, bytes_accessed=67_000_000, transcendentals=2_000_000),
        name="last",
    )(lens, left, h, acc, u, wd)
    return new_up, new_dn, y


def solution(mesh):
    up_spec = P("side", None, "rep", None)
    down_spec = P("side", None, None, "rep")
    act_spec = P("side", "rep", None)

    def device_step(w_up, w_down, g_up, g_down, learn_rate, prompts, prompt_lens):
        _, left, h, acc, u, _, wd = mlp_stack(
            learn_rate.reshape(1), prompt_lens, w_up, g_up, w_down, g_down, prompts[0]
        )
        return last_step(prompt_lens, left, h, acc, u, wd, w_up.shape, w_down.shape, prompts.shape)

    return jax.shard_map(
        device_step,
        mesh=mesh,
        in_specs=(up_spec, down_spec, up_spec, down_spec, P(), act_spec, P("rep")),
        out_specs=(up_spec, down_spec, act_spec),
        check_vma=False,
    )
```
